16 devices in a mesh: dp: 4 (over z, y), ep: 4 (over x, core).
Axes of the slice: x: 2, y: 2, z: 2, core: 2. Of those that a mesh axis runs over, the one named last changes fastest.
Arguments:
- x_in: bfloat16 [32768, 512], P(('dp', 'ep')), parts along dimension 0
- grad_y: bfloat16 [32768, 512], P(('dp', 'ep')), parts along dimension 0
- ids_a: int32 [32768, 2], P(('dp', 'ep')), parts along dimension 0
- gate_a: float32 [32768, 2], P(('dp', 'ep')), parts along dimension 0
- ids_b: int32 [32768, 2], P(('dp', 'ep')), parts along dimension 0
- gate_b: float32 [32768, 2], P(('dp', 'ep')), parts along dimension 0
- w1_a: bfloat16 [8, 512, 1792], P('ep')
- w3_a: bfloat16 [8, 512, 1792], P('ep')
- w2_a: bfloat16 [8, 1792, 512], P('ep')
- w1_b: bfloat16 [8, 512, 1792], P('ep')
- w3_b: bfloat16 [8, 512, 1792], P('ep')
- w2_b: bfloat16 [8, 1792, 512], P('ep')
- wg_mid: bfloat16 [512, 1792], replicated
- wu_mid: bfloat16 [512, 1792], replicated
- wd_mid: bfloat16 [1792, 512], replicated
- wg_top: bfloat16 [512, 1792], replicated
- wu_top: bfloat16 [512, 1792], replicated
- wd_top: bfloat16 [1792, 512], replicated
Outputs:
- output 1: bfloat16 [32768, 512], P(('dp', 'ep')), parts along dimension 0
- output 2: bfloat16 [32768, 512], P(('dp', 'ep')), parts along dimension 0
- output 3: float32 [32, 512, 1792], P(('dp', 'ep')), parts along dimension 0
- output 4: float32 [32, 512, 1792], P(('dp', 'ep')), parts along dimension 0
- output 5: float32 [32, 1792, 512], P(('dp', 'ep')), parts along dimension 0
- output 6: float32 [32, 512, 1792], P(('dp', 'ep')), parts along dimension 0
- output 7: float32 [32, 512, 1792], P(('dp', 'ep')), parts along dimension 0
- output 8: float32 [32, 1792, 512], P(('dp', 'ep')), parts along dimension 0
- output 9: float32 [32768, 2], P(('dp', 'ep')), parts along dimension 0
- output 10: float32 [32768, 2], P(('dp', 'ep')), parts along dimension 0
There are 4 independent parts. The reference program is written for one: setup_inputs(seed, part) draws one part's arguments, and reference() takes and returns one part's arrays. A program takes and returns all parts, laid end to end along the dimension named above; an argument that names none is the same for every part.
All inputs are finite; a program needn't handle non-finite values.
Results may differ from the reference program's by a relative error of at most 0.02.
Values are sent between devices in bfloat16 or wider.
A program may use at most 1 GiB of HBM per device.

```python
import jax
import jax.numpy as jnp
from jax import lax

HIDDEN = 512
EXPERT_FF = 1792
EXPERTS = 8
TOP_K = 2
DENSE_FF = 1792
TOKENS = 2048
GROUP_SIZE = 4
CAPACITY = 2 * TOKENS * TOP_K // EXPERTS
PART_ROWS = GROUP_SIZE * TOKENS


def draw_routing(key):
    half_load = TOKENS * TOP_K // EXPERTS

    def one_device(dev_key):
        key_order, key_spread, key_rows = jax.random.split(dev_key, 3)
        order = jax.random.permutation(key_order, EXPERTS)
        spread = jax.random.randint(key_spread, ((EXPERTS - 4) // 2,), 0, half_load)
        paired = jnp.stack([half_load + spread, half_load - spread], axis=1).reshape(-1)
        leading = jnp.array([2 * half_load, half_load // 2, half_load // 2, half_load], jnp.int32)
        by_rank = jnp.concatenate([leading, paired.astype(jnp.int32)])
        counts = jnp.zeros((EXPERTS,), jnp.int32).at[order].set(by_rank)
        sequence = jnp.repeat(jnp.arange(EXPERTS, dtype=jnp.int32), counts, total_repeat_length=TOKENS * TOP_K)
        table = sequence.reshape(TOP_K, TOKENS).T
        return table[jax.random.permutation(key_rows, TOKENS)]

    return jax.vmap(one_device)(jax.random.split(key, GROUP_SIZE)).reshape(PART_ROWS, TOP_K)


def setup_inputs(seed: int = 0, part: int = 0) -> dict:
    keys = jax.random.split(jax.random.key(seed), 18)

    def own(index):
        return jax.random.fold_in(keys[index], part)

    def normal(key, shape, scale):
        return (jax.random.normal(key, shape, jnp.float32) * scale).astype(jnp.bfloat16)

    def gates(key):
        return jax.random.uniform(key, (PART_ROWS, TOP_K), jnp.float32, 0.5, 1.5) * TOP_K ** -0.5

    expert_in = (EXPERTS, HIDDEN, EXPERT_FF)
    expert_out = (EXPERTS, EXPERT_FF, HIDDEN)
    return {
        'x_in': normal(own(0), (PART_ROWS, HIDDEN), 1.0),
        'grad_y': normal(own(1), (PART_ROWS, HIDDEN), 1.0),
        'ids_a': draw_routing(own(2)),
        'gate_a': gates(own(3)),
        'ids_b': draw_routing(own(4)),
        'gate_b': gates(own(5)),
        'w1_a': normal(keys[6], expert_in, HIDDEN ** -0.5),
        'w3_a': normal(keys[7], expert_in, HIDDEN ** -0.5),
        'w2_a': normal(keys[8], expert_out, EXPERT_FF ** -0.5),
        'w1_b': normal(keys[9], expert_in, HIDDEN ** -0.5),
        'w3_b': normal(keys[10], expert_in, HIDDEN ** -0.5),
        'w2_b': normal(keys[11], expert_out, EXPERT_FF ** -0.5),
        'wg_mid': normal(keys[12], (HIDDEN, DENSE_FF), HIDDEN ** -0.5),
        'wu_mid': normal(keys[13], (HIDDEN, DENSE_FF), HIDDEN ** -0.5),
        'wd_mid': normal(keys[14], (DENSE_FF, HIDDEN), DENSE_FF ** -0.5),
        'wg_top': normal(keys[15], (HIDDEN, DENSE_FF), HIDDEN ** -0.5),
        'wu_top': normal(keys[16], (HIDDEN, DENSE_FF), HIDDEN ** -0.5),
        'wd_top': normal(keys[17], (DENSE_FF, HIDDEN), DENSE_FF ** -0.5),
    }


def bf16_cast(values):
    return values.astype(jnp.bfloat16).astype(jnp.float32)


def pair_rows(expert_ids):
    per_dev = expert_ids.reshape(GROUP_SIZE, TOKENS * TOP_K)
    onehot = (per_dev[:, :, None] == jnp.arange(EXPERTS, dtype=jnp.int32)).astype(jnp.int32)
    slots = jnp.sum((jnp.cumsum(onehot, axis=1) - onehot) * onehot, axis=2)
    source = jnp.arange(GROUP_SIZE, dtype=jnp.int32)[:, None]
    return ((per_dev * GROUP_SIZE + source) * CAPACITY + slots).reshape(-1)


def moe_layer(x_rows, gate, rows_of_pairs, w_one, w_three, w_two):
    repeated = jnp.broadcast_to(x_rows[:, None, :], (PART_ROWS, TOP_K, HIDDEN)).reshape(-1, HIDDEN)
    staged = jnp.zeros((EXPERTS * GROUP_SIZE * CAPACITY, HIDDEN), jnp.float32).at[rows_of_pairs].set(repeated)

    def one_expert(operands):
        tokens, mat_one, mat_three, mat_two = operands
        pre_gate = jnp.dot(tokens, mat_one, preferred_element_type=jnp.float32)
        pre_up = jnp.dot(tokens, mat_three, preferred_element_type=jnp.float32)
        hidden = bf16_cast(jax.nn.silu(pre_gate) * pre_up)
        return bf16_cast(jnp.dot(hidden, mat_two, preferred_element_type=jnp.float32))

    outputs = lax.map(one_expert, (staged.reshape(EXPERTS, GROUP_SIZE * CAPACITY, HIDDEN), w_one, w_three, w_two))
    pairs = outputs.reshape(-1, HIDDEN)[rows_of_pairs].reshape(PART_ROWS, TOP_K, HIDDEN)
    return bf16_cast(x_rows + jnp.sum(gate[:, :, None] * pairs, axis=1))


def dense_block(x_rows, w_gate, w_up, w_down):
    def one_device(rows):
        pre_gate = jnp.dot(rows, w_gate, preferred_element_type=jnp.float32)
        pre_up = jnp.dot(rows, w_up, preferred_element_type=jnp.float32)
        hidden = bf16_cast(jax.nn.silu(pre_gate) * pre_up)
        return bf16_cast(rows + jnp.dot(hidden, w_down, preferred_element_type=jnp.float32))

    return lax.map(one_device, x_rows.reshape(GROUP_SIZE, TOKENS, HIDDEN)).reshape(PART_ROWS, HIDDEN)


def reference(x_in, grad_y, ids_a, gate_a, ids_b, gate_b, w1_a, w3_a, w2_a, w1_b, w3_b, w2_b, wg_mid, wu_mid, wd_mid, wg_top, wu_top, wd_top):
    rows_a = pair_rows(ids_a)
    rows_b = pair_rows(ids_b)
    dense_mid = (wg_mid.astype(jnp.float32), wu_mid.astype(jnp.float32), wd_mid.astype(jnp.float32))
    dense_top = (wg_top.astype(jnp.float32), wu_top.astype(jnp.float32), wd_top.astype(jnp.float32))

    def forward(x_start, mix_a, mix_b, one_a, three_a, two_a, one_b, three_b, two_b):
        x_a = moe_layer(x_start, mix_a, rows_a, one_a, three_a, two_a)
        x_mid = dense_block(x_a, dense_mid[0], dense_mid[1], dense_mid[2])
        x_b = moe_layer(x_mid, mix_b, rows_b, one_b, three_b, two_b)
        return dense_block(x_b, dense_top[0], dense_top[1], dense_top[2])

    y_out, pullback = jax.vjp(forward, x_in.astype(jnp.float32), gate_a, gate_b,
                              w1_a.astype(jnp.float32), w3_a.astype(jnp.float32), w2_a.astype(jnp.float32),
                              w1_b.astype(jnp.float32), w3_b.astype(jnp.float32), w2_b.astype(jnp.float32))
    grads = pullback(grad_y.astype(jnp.float32))
    return (y_out.astype(jnp.bfloat16), grads[0].astype(jnp.bfloat16), grads[3], grads[4], grads[5],
            grads[6], grads[7], grads[8], grads[1], grads[2])
```

```python
import functools

import jax
import jax.numpy as jnp
from jax import lax
from jax.experimental import pallas as pl
from jax.experimental.pallas import tpu as pltpu
from jax.sharding import PartitionSpec as P


F32 = jnp.float32
BF16 = jnp.bfloat16
SUB = 128
WIN = SUB + 16
ROWS = 256
TOK = 256
CHUNK = 256
PACK = 1024
VMEM_LIMIT = 62 * 1024 * 1024

MM = (((1,), (0,)), ((), ()))
LAST = (((1,), (1,)), ((), ()))
FIRST = (((0,), (0,)), ((), ()))


def dot(left, right, dims=MM):
    return lax.dot_general(left, right, dims, preferred_element_type=F32)


def params():
    return pltpu.CompilerParams(dimension_semantics=("arbitrary",), vmem_limit_bytes=VMEM_LIMIT)


def cost(flops, bytes_accessed):
    return pl.CostEstimate(flops=flops, bytes_accessed=bytes_accessed, transcendentals=0)


def route(ids, gate, experts):
    first = ids[..., None, :, 0] == experts[:, None]
    second = ids[..., None, :, 1] == experts[:, None]
    hit = (first | second).astype(jnp.int32)
    ends = jnp.cumsum(hit, axis=-1)
    before = ends - hit
    slots = jnp.where(hit > 0, before, -1)
    gates = jnp.where(first, gate[..., None, :, 0], 0.0) + jnp.where(second, gate[..., None, :, 1], 0.0)
    return slots, gates, before[..., ::SUB], ends[..., -1]


def combine_rows(index, local, win_ref, slots_ref, gates_ref, backs, capacity):
    n_local = len(backs)
    n_exp = slots_ref.shape[1]
    column = lax.broadcasted_iota(jnp.int32, (SUB, WIN), 1)
    tokens = pl.ds(local * SUB, SUB)
    slots = slots_ref[tokens, :]
    gates = None if gates_ref is None else gates_ref[tokens, :]
    total = None
    for exp in range(n_exp):
        start = win_ref[index * n_exp + exp]
        where = slots[:, exp:exp + 1] - start
        pick = jnp.where(column == where, 1.0, 0.0).astype(BF16)
        source = pl.ds(pl.multiple_of(exp // n_local * capacity + start, 16), WIN)
        term = dot(pick, backs[exp % n_local][source, :])
        if gates is not None:
            term = term * gates[:, exp:exp + 1]
        total = term if total is None else total + term
    return total


def zero_all(refs):
    for ref in refs:
        ref[...] = jnp.zeros(ref.shape, ref.dtype)


def swiglu_grads(pre_gate, pre_up, sigma, grad_hidden):
    grad_up = grad_hidden * (pre_gate * sigma)
    grad_gate = grad_hidden * pre_up * sigma * (1.0 + pre_gate * (1.0 - sigma))
    return grad_gate.astype(BF16), grad_up.astype(BF16)


def forward_kernel(capacity, win_in, x_ref, slots_in, gates_in, back0, back1, wg_ref, wu_ref, wd_ref,
                   mix_ref, out_ref, hid_ref):
    step = pl.program_id(0)
    for sub in range(TOK // SUB):
        part = slice(sub * SUB, (sub + 1) * SUB)
        total = combine_rows(step * (TOK // SUB) + sub, sub, win_in, slots_in, gates_in, (back0, back1), capacity)
        mix_ref[part, :] = (x_ref[part, :].astype(F32) + total).astype(BF16)
    rows = mix_ref[...]
    for at in range(0, wg_ref.shape[1], CHUNK):
        cols = slice(at, at + CHUNK)
        pre_gate = dot(rows, wg_ref[:, cols])
        pre_up = dot(rows, wu_ref[:, cols])
        hid_ref[:, cols] = (pre_gate * jax.nn.sigmoid(pre_gate) * pre_up).astype(BF16)
    out_ref[...] = (rows.astype(F32) + dot(hid_ref[...], wd_ref[...])).astype(BF16)


def top_kernel(capacity, win_in, x_ref, gy_ref, slots_in, gates_in, back0, back1, wg_ref, wu_ref, wd_ref,
               y_ref, grad_ref, hid_ref, dg_ref, du_ref, mix_ref):
    step = pl.program_id(0)
    for sub in range(TOK // SUB):
        part = slice(sub * SUB, (sub + 1) * SUB)
        total = combine_rows(step * (TOK // SUB) + sub, sub, win_in, slots_in, gates_in, (back0, back1), capacity)
        mix_ref[part, :] = (x_ref[part, :].astype(F32) + total).astype(BF16)
    rows = mix_ref[...]
    grad = gy_ref[...]
    for at in range(0, wg_ref.shape[1], CHUNK):
        cols = slice(at, at + CHUNK)
        pre_gate = dot(rows, wg_ref[:, cols])
        pre_up = dot(rows, wu_ref[:, cols])
        sigma = jax.nn.sigmoid(pre_gate)
        hid_ref[:, cols] = (pre_gate * sigma * pre_up).astype(BF16)
        grad_hidden = dot(grad, wd_ref[cols, :], LAST)
        dg_ref[:, cols], du_ref[:, cols] = swiglu_grads(pre_gate, pre_up, sigma, grad_hidden)
    y_ref[...] = (rows.astype(F32) + dot(hid_ref[...], wd_ref[...])).astype(BF16)
    branch = dot(dg_ref[...], wg_ref[...], LAST) + dot(du_ref[...], wu_ref[...], LAST)
    grad_ref[...] = (grad.astype(F32) + branch).astype(BF16)


def backward_kernel(capacity, win_in, g_ref, x_ref, slots_in, back0, back1, wg_ref, wu_ref, wd_ref,
                    grad_ref, dg_ref, du_ref, mix_ref):
    step = pl.program_id(0)
    for sub in range(TOK // SUB):
        part = slice(sub * SUB, (sub + 1) * SUB)
        total = combine_rows(step * (TOK // SUB) + sub, sub, win_in, slots_in, None, (back0, back1), capacity)
        mix_ref[part, :] = (g_ref[part, :].astype(F32) + total).astype(BF16)
    rows = x_ref[...]
    grad = mix_ref[...]
    for at in range(0, wg_ref.shape[1], CHUNK):
        cols = slice(at, at + CHUNK)
        pre_gate = dot(rows, wg_ref[:, cols])
        pre_up = dot(rows, wu_ref[:, cols])
        sigma = jax.nn.sigmoid(pre_gate)
        grad_hidden = dot(grad, wd_ref[cols, :], LAST)
        dg_ref[:, cols], du_ref[:, cols] = swiglu_grads(pre_gate, pre_up, sigma, grad_hidden)
    branch = dot(dg_ref[...], wg_ref[...], LAST) + dot(du_ref[...], wu_ref[...], LAST)
    grad_ref[...] = (grad.astype(F32) + branch).astype(BF16)


def final_kernel(capacity, win_in, g_ref, slots_in, back0, back1, out_ref):
    step = pl.program_id(0)
    for sub in range(TOK // SUB):
        part = slice(sub * SUB, (sub + 1) * SUB)
        total = combine_rows(step * (TOK // SUB) + sub, sub, win_in, slots_in, None, (back0, back1), capacity)
        out_ref[part, :] = (g_ref[part, :].astype(F32) + total).astype(BF16)


def pack_kernel(n_local, with_gates, win_ref, x_ref, slots_ref, *refs):
    gates_ref, refs = (refs[0], refs[1:]) if with_gates else (None, refs)
    sends, columns = refs[:n_local], refs[n_local:]
    step = pl.program_id(0)

    @pl.when(step == 0)
    def _():
        zero_all(refs)

    line = lax.broadcasted_iota(jnp.int32, (WIN, SUB), 0)
    subs = PACK // SUB

    def moved(sub):
        part = slice(sub * SUB, (sub + 1) * SUB)
        rows = x_ref[part, :]
        found = []
        for loc in range(n_local):
            window = (step * subs + sub) * n_local + loc
            match = line == slots_ref[loc:loc + 1, part] - win_ref[2 * window]
            target = pl.ds(pl.multiple_of(win_ref[2 * window + 1], 16), WIN)
            gate = jnp.where(match, gates_ref[loc:loc + 1, part], 0.0) if with_gates else None
            found.append((target, dot(jnp.where(match, 1.0, 0.0).astype(BF16), rows), gate))
        return found

    ready = moved(0)
    for sub in range(subs):
        following = moved(sub + 1) if sub + 1 < subs else None
        for loc, (target, rows, gate) in enumerate(ready):
            sends[loc][target, :] = (sends[loc][target, :].astype(F32) + rows).astype(BF16)
            if with_gates:
                columns[loc][target, :] += gate
        ready = following


def spread(meta, source, target, capacity):
    for src in range(target.shape[0] // capacity):
        at = pl.ds(pl.multiple_of(meta[1 + src], 16), capacity)
        target[src * capacity:(src + 1) * capacity, :] = source[at, :]


def expert_forward_kernel(capacity, meta, x_ref, w1_ref, w3_ref, w2_ref, o_ref, all_ref, hid_ref):
    step = pl.program_id(0)

    @pl.when(step == 0)
    def _():
        zero_all((all_ref,))

    @pl.when(step < meta[0])
    def _():
        rows = x_ref[...]
        for at in range(0, w1_ref.shape[1], CHUNK):
            cols = slice(at, at + CHUNK)
            pre_gate = dot(rows, w1_ref[:, cols])
            pre_up = dot(rows, w3_ref[:, cols])
            hid_ref[:, cols] = (pre_gate * jax.nn.sigmoid(pre_gate) * pre_up).astype(BF16)
        block = pl.ds(pl.multiple_of(step * ROWS, ROWS), ROWS)
        all_ref[block, :] = dot(hid_ref[...], w2_ref[...]).astype(BF16)

    @pl.when(step == pl.num_programs(0) - 1)
    def _():
        spread(meta, all_ref, o_ref, capacity)


def expert_backward_kernel(capacity, n_local, loc, meta, win_ref, x_ref, c_ref, gcol_ref, slots_ref,
                           w1_ref, w3_ref, w2_ref, dx_ref, dgate_ref, hid_ref, dg_ref, du_ref, all_ref, dcol_ref):
    step = pl.program_id(0)

    @pl.when(step == 0)
    def _():
        zero_all((all_ref, dcol_ref))

    @pl.when(step < meta[0])
    def _():
        block = pl.ds(pl.multiple_of(step * ROWS, ROWS), ROWS)
        rows = x_ref[...]
        grad = c_ref[...]
        gate = jnp.sum(gcol_ref[...], axis=1, keepdims=True)
        partial = jnp.zeros((ROWS, 128), F32)
        for at in range(0, w1_ref.shape[1], CHUNK):
            cols = slice(at, at + CHUNK)
            pre_gate = dot(rows, w1_ref[:, cols])
            pre_up = dot(rows, w3_ref[:, cols])
            sigma = jax.nn.sigmoid(pre_gate)
            hidden = (pre_gate * sigma * pre_up).astype(BF16)
            hid_ref[:, cols] = hidden
            back = dot(grad, w2_ref[cols, :], LAST)
            product = hidden.astype(F32) * back
            for lane in range(0, CHUNK, 128):
                partial += product[:, lane:lane + 128]
            dg_ref[:, cols], du_ref[:, cols] = swiglu_grads(pre_gate, pre_up, sigma, back * gate)
        dcol_ref[block, :] = partial
        all_ref[block, :] = (dot(dg_ref[...], w1_ref[...], LAST) + dot(du_ref[...], w3_ref[...], LAST)).astype(BF16)

    @pl.when(step == pl.num_programs(0) - 1)
    def _():
        spread(meta, all_ref, dx_ref, capacity)
        line = lax.broadcasted_iota(jnp.int32, (WIN, SUB), 0)
        n_src, n_tok = dgate_ref.shape
        for src in range(n_src):
            def body(sub, _):
                window = (src * (n_tok // SUB) + sub) * n_local + loc
                part = pl.ds(pl.multiple_of(sub * SUB, SUB), SUB)
                where = slots_ref[src:src + 1, part] - win_ref[2 * window]
                source = pl.ds(pl.multiple_of(win_ref[2 * window + 1], 16), WIN)
                values = jnp.sum(dcol_ref[source, :], axis=1, keepdims=True)
                dgate_ref[src:src + 1, part] = jnp.sum(jnp.where(line == where, values, 0.0), axis=0, keepdims=True)
                return 0

            lax.fori_loop(0, n_tok // SUB, body, 0)


def expert_weights_kernel(n_alias, meta, x_ref, c_ref, gcol_ref, hid_ref, dg_ref, du_ref, *refs):
    dw1_ref, dw3_ref, dw2_ref = refs[n_alias:]
    step = pl.program_id(0)

    @pl.when(step == 0)
    def _():
        zero_all((dw1_ref, dw3_ref, dw2_ref))

    @pl.when(step < meta[0])
    def _():
        gate = jnp.sum(gcol_ref[...], axis=1, keepdims=True)
        scaled = (c_ref[...].astype(F32) * gate).astype(BF16)
        rows = x_ref[...]
        dw1_ref[...] += dot(rows, dg_ref[...], FIRST)
        dw3_ref[...] += dot(rows, du_ref[...], FIRST)
        dw2_ref[...] += dot(hid_ref[...], scaled, FIRST)


def solution(mesh):
    group = mesh.shape['ep']
    tok_spec = P(('dp', 'ep'), None)
    exp_spec = P('ep', None, None)
    full_spec = P(None, None)
    grad_spec = P(('dp', 'ep'), None, None)
    buffered = pl.Buffered(buffer_count=1)

    def layer_program(x_in, grad_y, ids_a, gate_a, ids_b, gate_b, w1_a, w3_a, w2_a, w1_b, w3_b, w2_b,
                       wg_mid, wu_mid, wd_mid, wg_top, wu_top, wd_top):
        n_tok, dim = x_in.shape
        n_local, _, ff = w1_a.shape
        n_exp = n_local * group
        capacity = 2 * n_tok * ids_a.shape[1] // n_exp
        n_rows = group * capacity
        me = lax.axis_index('ep')

        tile = pl.BlockSpec((TOK, dim), lambda i, *_: (i, 0))
        col_tile = pl.BlockSpec((TOK, n_exp), lambda i, *_: (i, 0))
        whole = pl.BlockSpec((n_rows, dim), lambda i, *_: (0, 0), pipeline_mode=buffered)
        w_in = pl.BlockSpec((dim, ff), lambda i, *_: (0, 0), pipeline_mode=buffered)
        w_out = pl.BlockSpec((ff, dim), lambda i, *_: (0, 0), pipeline_mode=buffered)
        rows_shape = jax.ShapeDtypeStruct((n_tok, dim), BF16)
        buffer_shape = jax.ShapeDtypeStruct((n_rows, dim), BF16)
        wide = pltpu.VMEM((TOK, ff), BF16)
        narrow = pltpu.VMEM((TOK, dim), BF16)
        unit_flops = 2 * n_tok * dim * ff

        def token_call(kernel, in_specs, out_specs, out_shape, scratch, matmuls):
            return pl.pallas_call(
                functools.partial(kernel, capacity),
                grid_spec=pltpu.PrefetchScalarGridSpec(
                    num_scalar_prefetch=1, grid=(n_tok // TOK,), in_specs=in_specs, out_specs=out_specs,
                    scratch_shapes=scratch),
                out_shape=out_shape, compiler_params=params(),
                cost_estimate=cost(int(matmuls * unit_flops), 20 * 2**20))

        forward = token_call(forward_kernel, [tile, col_tile, col_tile, whole, whole, w_in, w_in, w_out],
                             [tile, tile], [rows_shape, rows_shape], [wide], 5)
        top = token_call(top_kernel, [tile, tile, col_tile, col_tile, whole, whole, w_in, w_in, w_out],
                         [tile, tile], [rows_shape, rows_shape], [wide, wide, wide, narrow], 8)
        backward = token_call(backward_kernel, [tile, tile, col_tile, whole, whole, w_in, w_in, w_out],
                              tile, rows_shape, [wide, wide, narrow], 7)
        final = token_call(final_kernel, [tile, col_tile, whole, whole], tile, rows_shape, [], 1)

        n_blocks = n_rows // ROWS
        tiles = n_tok // PACK
        pack_tile = pl.BlockSpec((PACK, dim), lambda i, *_: (i, 0))
        line = pl.BlockSpec((None, n_local, PACK), lambda i, *_: (i // tiles, 0, i % tiles))
        column_shape = jax.ShapeDtypeStruct((n_rows, 128), F32)
        column = pl.BlockSpec((n_rows, 128), lambda i, *_: (0, 0), pipeline_mode=buffered)

        def pack(windows, tokens, slots, gates=None):
            with_gates = gates is not None
            return pl.pallas_call(
                functools.partial(pack_kernel, n_local, with_gates),
                grid_spec=pltpu.PrefetchScalarGridSpec(
                    num_scalar_prefetch=1, grid=(group * tiles,),
                    in_specs=[pack_tile, line] + [line] * with_gates,
                    out_specs=[whole] * n_local + [column] * (n_local * with_gates)),
                out_shape=[buffer_shape] * n_local + [column_shape] * (n_local * with_gates),
                compiler_params=params(), cost_estimate=cost(2 * unit_flops, 20 * 2**20),
            )(windows, tokens, slots, *((gates,) if with_gates else ()))

        def row_block(i, meta, *_):
            return (jnp.maximum(jnp.minimum(i, meta[0] - 1), 0), 0)

        def expert_specs(loc):
            return (pl.BlockSpec((ROWS, dim), row_block),
                    pl.BlockSpec((None, dim, ff), lambda i, *_: (loc, 0, 0), pipeline_mode=buffered),
                    pl.BlockSpec((None, ff, dim), lambda i, *_: (loc, 0, 0), pipeline_mode=buffered))

        def expert_forward(loc, meta, tokens, w1, w3, w2):
            block, e_in, e_out = expert_specs(loc)
            return pl.pallas_call(
                functools.partial(expert_forward_kernel, capacity),
                grid_spec=pltpu.PrefetchScalarGridSpec(
                    num_scalar_prefetch=1, grid=(n_blocks,), in_specs=[block, e_in, e_in, e_out], out_specs=whole,
                    scratch_shapes=[pltpu.VMEM((n_rows, dim), BF16), pltpu.VMEM((ROWS, ff), BF16)]),
                out_shape=buffer_shape, compiler_params=params(),
                cost_estimate=cost(3 * unit_flops, 12 * 2**20))(meta, tokens, w1, w3, w2)

        hidden_block = pl.BlockSpec((ROWS, ff), row_block)
        hidden_shape = jax.ShapeDtypeStruct((n_rows, ff), BF16)

        def expert_backward(loc, meta, windows, tokens, grads, gates, slots, w1, w3, w2):
            block, e_in, e_out = expert_specs(loc)
            small = pl.BlockSpec((group, n_tok), lambda i, *_: (0, 0), pipeline_mode=buffered)
            return pl.pallas_call(
                functools.partial(expert_backward_kernel, capacity, n_local, loc),
                grid_spec=pltpu.PrefetchScalarGridSpec(
                    num_scalar_prefetch=2, grid=(n_blocks,),
                    in_specs=[block, block, pl.BlockSpec((ROWS, 128), row_block), small, e_in, e_in, e_out],
                    out_specs=[whole, small] + [hidden_block] * 3,
                    scratch_shapes=[pltpu.VMEM((n_rows, dim), BF16), pltpu.VMEM((n_rows, 128), F32)]),
                out_shape=[buffer_shape, jax.ShapeDtypeStruct((group, n_tok), F32)] + [hidden_shape] * 3,
                compiler_params=params(), cost_estimate=cost(5 * unit_flops, 60 * 2**20),
            )(meta, windows, tokens, grads, gates, slots, w1, w3, w2)

        def expert_weights(loc, meta, tokens, grads, gates, hidden, earlier):
            block, e_in, e_out = expert_specs(loc)
            n_alias = 0 if earlier is None else 3
            aliases = {} if earlier is None else {7: 0, 8: 1, 9: 2}
            extra = () if earlier is None else tuple(earlier)
            return pl.pallas_call(
                functools.partial(expert_weights_kernel, n_alias),
                grid_spec=pltpu.PrefetchScalarGridSpec(
                    num_scalar_prefetch=1, grid=(n_blocks,),
                    in_specs=([block, block, pl.BlockSpec((ROWS, 128), row_block)] + [hidden_block] * 3
                              + [pl.BlockSpec(memory_space=pl.ANY)] * n_alias),
                    out_specs=[e_in, e_in, e_out]),
                out_shape=[jax.ShapeDtypeStruct((n_local, dim, ff), F32), jax.ShapeDtypeStruct((n_local, dim, ff), F32),
                           jax.ShapeDtypeStruct((n_local, ff, dim), F32)],
                input_output_aliases=aliases, compiler_params=params(),
                cost_estimate=cost(3 * unit_flops, 60 * 2**20),
            )(meta, tokens, grads, gates, *hidden, *extra)

        ids_both, gates_both = jnp.stack([ids_a, ids_b]), jnp.stack([gate_a, gate_b])
        slots_here, gates_here, starts_here, _ = route(ids_both, gates_both, jnp.arange(n_exp, dtype=jnp.int32))
        windows_here = jnp.minimum(starts_here // 16 * 16, capacity - WIN)
        win_a, win_b = windows_here.transpose(0, 2, 1).reshape(2, -1)
        slots_col, gates_col = slots_here.transpose(0, 2, 1), gates_here.transpose(0, 2, 1)
        ids_all = lax.all_gather(ids_both, 'ep')
        gates_all = lax.all_gather(gates_both, 'ep')
        slots, gates, starts, counts = route(ids_all, gates_all, me * n_local + jnp.arange(n_local, dtype=jnp.int32))
        room = (counts + 15) // 16 * 16
        offsets = jnp.cumsum(room, axis=0) - room
        windows = jnp.minimum(starts // 16 * 16, capacity - WIN)
        windows = jnp.stack([windows, windows + offsets[..., None]], axis=-1)
        windows = windows.transpose(1, 0, 3, 2, 4).reshape(2, -1)
        n_used = (jnp.sum(room, axis=0) + ROWS - 1) // ROWS
        meta = jnp.concatenate([n_used[None], offsets], axis=0)

        def gather_rows(rows):
            return lax.all_gather(rows, 'ep', axis=0, tiled=True)

        def to_home(rows):
            return lax.all_to_all(rows.reshape(group, capacity, dim), 'ep', 0, 0, tiled=True).reshape(n_rows, dim)

        def moe_forward(tokens, layer, w1, w3, w2):
            backs = []
            for loc in range(n_local):
                rows = expert_forward(loc, meta[:, layer, loc], tokens[loc], w1, w3, w2)
                if backs:
                    rows, backs[-1] = lax.optimization_barrier((rows, backs[-1]))
                backs.append(to_home(rows))
            return backs

        def moe_backward(tokens, grads, layer, ids, w1, w3, w2):
            backs, dgates, kept, earlier = [], [], [], None
            packed = pack(windows[layer], grads, slots[:, layer], gates[:, layer])
            for loc in range(n_local):
                dx, dgate, *hidden = expert_backward(
                    loc, meta[:, layer, loc], windows[layer], tokens[loc], packed[loc], packed[n_local + loc],
                    slots[:, layer, loc], w1, w3, w2)
                if backs:
                    dx, backs[-1] = lax.optimization_barrier((dx, backs[-1]))
                backs.append(to_home(dx))
                dgates.append(dgate)
                kept.append(hidden)
            for loc in range(n_local):
                earlier = expert_weights(loc, meta[:, layer, loc], tokens[loc], packed[loc], packed[n_local + loc],
                                         kept[loc], earlier)
            dgates, backs = lax.optimization_barrier((jnp.stack(dgates, axis=1), backs))
            home = lax.all_to_all(dgates, 'ep', 0, 0, tiled=True)
            experts = jnp.arange(n_exp, dtype=jnp.int32)[:, None, None]
            dgate = jnp.sum(jnp.where(ids[None] == experts, home.reshape(n_exp, n_tok)[:, :, None], 0.0), axis=0)
            return backs, dgate, earlier

        tokens_a = pack(windows[0], gather_rows(x_in), slots[:, 0])
        backs_a = moe_forward(tokens_a, 0, w1_a, w3_a, w2_a)
        x_a, x_mid = forward(win_a, x_in, slots_col[0], gates_col[0], *backs_a, wg_mid, wu_mid, wd_mid)
        tokens_b = pack(windows[1], gather_rows(x_mid), slots[:, 1])
        backs_b = moe_forward(tokens_b, 1, w1_b, w3_b, w2_b)

        y_out, grad_b = top(win_b, x_mid, grad_y, slots_col[1], gates_col[1], *backs_b, wg_top, wu_top, wd_top)
        again, _ = lax.optimization_barrier((x_in, grad_b))
        backs_b, dgate_b, dw_b = moe_backward(tokens_b, gather_rows(grad_b), 1, ids_b, w1_b, w3_b, w2_b)
        tokens_a = pack(windows[0], gather_rows(again), slots[:, 0])
        grad_a = backward(win_b, grad_b, x_a, slots_col[1], *backs_b, wg_mid, wu_mid, wd_mid)
        backs_a, dgate_a, dw_a = moe_backward(tokens_a, gather_rows(grad_a), 0, ids_a, w1_a, w3_a, w2_a)
        dx_in = final(win_a, grad_a, slots_col[0], *backs_a)
        return (y_out, dx_in, *dw_a, *dw_b, dgate_a, dgate_b)

    in_specs = (tok_spec, tok_spec, tok_spec, tok_spec, tok_spec, tok_spec,
                exp_spec, exp_spec, exp_spec, exp_spec, exp_spec, exp_spec,
                full_spec, full_spec, full_spec, full_spec, full_spec, full_spec)
    out_specs = (tok_spec, tok_spec, grad_spec, grad_spec, grad_spec, grad_spec, grad_spec, grad_spec, tok_spec, tok_spec)
    return jax.shard_map(layer_program, mesh=mesh, in_specs=in_specs, out_specs=out_specs, check_vma=False)
```

```python
import functools

import jax
import jax.numpy as jnp
from jax import lax
from jax.experimental import pallas as pl
from jax.experimental.pallas import tpu as pltpu
from jax.sharding import PartitionSpec as P


F32 = jnp.float32
BF16 = jnp.bfloat16
SUB = 128
WIN = SUB + 16
ROWS = 256
TOK = 256
CHUNK = 256
PACK = 1024
VMEM_LIMIT = 62 * 1024 * 1024

MM = (((1,), (0,)), ((), ()))
LAST = (((1,), (1,)), ((), ()))
FIRST = (((0,), (0,)), ((), ()))


def dot(left, right, dims=MM):
    return lax.dot_general(left, right, dims, preferred_element_type=F32)


def params():
    return pltpu.CompilerParams(dimension_semantics=("arbitrary",), vmem_limit_bytes=VMEM_LIMIT)


def cost(flops, bytes_accessed):
    return pl.CostEstimate(flops=flops, bytes_accessed=bytes_accessed, transcendentals=0)


def route(ids, gate, experts):
    first = ids[..., None, :, 0] == experts[:, None]
    second = ids[..., None, :, 1] == experts[:, None]
    hit = (first | second).astype(jnp.int32)
    ends = jnp.cumsum(hit, axis=-1)
    before = ends - hit
    slots = jnp.where(hit > 0, before, -1)
    gates = jnp.where(first, gate[..., None, :, 0], 0.0) + jnp.where(second, gate[..., None, :, 1], 0.0)
    return slots, gates, before[..., ::SUB], ends[..., -1]


def combine_rows(index, local, win_ref, slots_ref, gates_ref, backs, capacity):
    n_local = len(backs)
    n_exp = slots_ref.shape[1]
    column = lax.broadcasted_iota(jnp.int32, (SUB, WIN), 1)
    tokens = pl.ds(local * SUB, SUB)
    slots = slots_ref[tokens, :]
    gates = None if gates_ref is None else gates_ref[tokens, :]
    total = None
    for exp in range(n_exp):
        start = win_ref[index * n_exp + exp]
        where = slots[:, exp:exp + 1] - start
        pick = jnp.where(column == where, 1.0, 0.0).astype(BF16)
        source = pl.ds(pl.multiple_of(exp // n_local * capacity + start, 16), WIN)
        term = dot(pick, backs[exp % n_local][source, :])
        if gates is not None:
            term = term * gates[:, exp:exp + 1]
        total = term if total is None else total + term
    return total


def zero_all(refs):
    for ref in refs:
        ref[...] = jnp.zeros(ref.shape, ref.dtype)


def swiglu_grads(pre_gate, pre_up, sigma, grad_hidden):
    grad_up = grad_hidden * (pre_gate * sigma)
    grad_gate = grad_hidden * pre_up * sigma * (1.0 + pre_gate * (1.0 - sigma))
    return grad_gate.astype(BF16), grad_up.astype(BF16)


def forward_kernel(capacity, win_in, x_ref, slots_in, gates_in, back0, back1, wg_ref, wu_ref, wd_ref,
                   mix_ref, out_ref, hid_ref):
    step = pl.program_id(0)
    for sub in range(TOK // SUB):
        part = slice(sub * SUB, (sub + 1) * SUB)
        total = combine_rows(step * (TOK // SUB) + sub, sub, win_in, slots_in, gates_in, (back0, back1), capacity)
        mix_ref[part, :] = (x_ref[part, :].astype(F32) + total).astype(BF16)
    rows = mix_ref[...]
    for at in range(0, wg_ref.shape[1], CHUNK):
        cols = slice(at, at + CHUNK)
        pre_gate = dot(rows, wg_ref[:, cols])
        pre_up = dot(rows, wu_ref[:, cols])
        hid_ref[:, cols] = (pre_gate * jax.nn.sigmoid(pre_gate) * pre_up).astype(BF16)
    out_ref[...] = (rows.astype(F32) + dot(hid_ref[...], wd_ref[...])).astype(BF16)


def top_kernel(capacity, win_in, x_ref, gy_ref, slots_in, gates_in, back, wg_ref, wu_ref, wd_ref,
               y_ref, grad_ref, hid_ref, dg_ref, du_ref, mix_ref):
    step = pl.program_id(0)
    for sub in range(TOK // SUB):
        part = slice(sub * SUB, (sub + 1) * SUB)
        total = combine_rows(step * (TOK // SUB) + sub, sub, win_in, slots_in, gates_in, (back,), capacity)
        mix_ref[part, :] = (x_ref[part, :].astype(F32) + total).astype(BF16)
    rows = mix_ref[...]
    grad = gy_ref[...]
    for at in range(0, wg_ref.shape[1], CHUNK):
        cols = slice(at, at + CHUNK)
        pre_gate = dot(rows, wg_ref[:, cols])
        pre_up = dot(rows, wu_ref[:, cols])
        sigma = jax.nn.sigmoid(pre_gate)
        hid_ref[:, cols] = (pre_gate * sigma * pre_up).astype(BF16)
        grad_hidden = dot(grad, wd_ref[cols, :], LAST)
        dg_ref[:, cols], du_ref[:, cols] = swiglu_grads(pre_gate, pre_up, sigma, grad_hidden)
    y_ref[...] = (rows.astype(F32) + dot(hid_ref[...], wd_ref[...])).astype(BF16)
    branch = dot(dg_ref[...], wg_ref[...], LAST) + dot(du_ref[...], wu_ref[...], LAST)
    grad_ref[...] = (grad.astype(F32) + branch).astype(BF16)


def backward_kernel(capacity, win_in, g_ref, x_ref, slots_in, back0, back1, wg_ref, wu_ref, wd_ref,
                    grad_ref, dg_ref, du_ref, mix_ref):
    step = pl.program_id(0)
    for sub in range(TOK // SUB):
        part = slice(sub * SUB, (sub + 1) * SUB)
        total = combine_rows(step * (TOK // SUB) + sub, sub, win_in, slots_in, None, (back0, back1), capacity)
        mix_ref[part, :] = (g_ref[part, :].astype(F32) + total).astype(BF16)
    rows = x_ref[...]
    grad = mix_ref[...]
    for at in range(0, wg_ref.shape[1], CHUNK):
        cols = slice(at, at + CHUNK)
        pre_gate = dot(rows, wg_ref[:, cols])
        pre_up = dot(rows, wu_ref[:, cols])
        sigma = jax.nn.sigmoid(pre_gate)
        grad_hidden = dot(grad, wd_ref[cols, :], LAST)
        dg_ref[:, cols], du_ref[:, cols] = swiglu_grads(pre_gate, pre_up, sigma, grad_hidden)
    branch = dot(dg_ref[...], wg_ref[...], LAST) + dot(du_ref[...], wu_ref[...], LAST)
    grad_ref[...] = (grad.astype(F32) + branch).astype(BF16)


def final_kernel(capacity, win_in, g_ref, slots_in, back0, back1, out_ref):
    step = pl.program_id(0)
    for sub in range(TOK // SUB):
        part = slice(sub * SUB, (sub + 1) * SUB)
        total = combine_rows(step * (TOK // SUB) + sub, sub, win_in, slots_in, None, (back0, back1), capacity)
        out_ref[part, :] = (g_ref[part, :].astype(F32) + total).astype(BF16)


def pack_kernel(n_local, n_sends, with_gates, win_ref, x_ref, slots_ref, *refs):
    gates_ref, refs = (refs[0], refs[1:]) if with_gates else (None, refs)
    sends, columns = refs[:n_sends], refs[n_sends:]
    step = pl.program_id(0)

    @pl.when(step == 0)
    def _():
        zero_all(refs)

    line = lax.broadcasted_iota(jnp.int32, (WIN, SUB), 0)
    subs = PACK // SUB

    def moved(sub):
        part = slice(sub * SUB, (sub + 1) * SUB)
        rows = x_ref[part, :]
        found = []
        for loc in range(n_local):
            window = (step * subs + sub) * n_local + loc
            match = line == slots_ref[loc:loc + 1, part] - win_ref[2 * window]
            target = pl.ds(pl.multiple_of(win_ref[2 * window + 1], 16), WIN)
            gate = jnp.where(match, gates_ref[loc:loc + 1, part], 0.0) if with_gates else None
            found.append((target, dot(jnp.where(match, 1.0, 0.0).astype(BF16), rows), gate))
        return found

    ready = moved(0)
    for sub in range(subs):
        following = moved(sub + 1) if sub + 1 < subs else None
        for loc, (target, rows, gate) in enumerate(ready):
            send = sends[loc % n_sends]
            send[target, :] = (send[target, :].astype(F32) + rows).astype(BF16)
            if with_gates:
                columns[loc][target, :] += gate
        ready = following


def spread(meta, source, target, capacity):
    for src in range(target.shape[0] // capacity):
        at = pl.ds(pl.multiple_of(meta[1 + src], 16), capacity)
        target[src * capacity:(src + 1) * capacity, :] = source[at, :]


def expert_forward_kernel(capacity, meta, x_ref, w1_ref, w3_ref, w2_ref, o_ref, all_ref, hid_ref):
    step = pl.program_id(0)

    @pl.when(step == 0)
    def _():
        zero_all((all_ref,))

    @pl.when(step < meta[0])
    def _():
        rows = x_ref[...]
        for at in range(0, w1_ref.shape[1], CHUNK):
            cols = slice(at, at + CHUNK)
            pre_gate = dot(rows, w1_ref[:, cols])
            pre_up = dot(rows, w3_ref[:, cols])
            hid_ref[:, cols] = (pre_gate * jax.nn.sigmoid(pre_gate) * pre_up).astype(BF16)
        block = pl.ds(pl.multiple_of(step * ROWS, ROWS), ROWS)
        all_ref[block, :] = dot(hid_ref[...], w2_ref[...]).astype(BF16)

    @pl.when(step == pl.num_programs(0) - 1)
    def _():
        spread(meta, all_ref, o_ref, capacity)


def all_experts_kernel(capacity, plan, x_ref, w1_ref, w3_ref, w2_ref, o_ref, hid_ref):
    step = pl.program_id(0)
    parts, depth, ff = w1_ref.shape
    out_depth, dim = w2_ref.shape[1:]

    @pl.when(step == 0)
    def _():
        zero_all((o_ref,))

    @pl.when(step < plan[0])
    def _():
        rows = x_ref[...]
        for at in range(0, ff, CHUNK):
            cols = slice(at, at + CHUNK)
            pre_gate = dot(rows, w1_ref[:, :, cols].reshape(parts * depth, CHUNK))
            pre_up = dot(rows, w3_ref[:, :, cols].reshape(parts * depth, CHUNK))
            hid_ref[:, cols] = (pre_gate * jax.nn.sigmoid(pre_gate) * pre_up).astype(BF16)
        at = plan[1 + 2 * step] * capacity + plan[2 + 2 * step] * ROWS
        o_ref[pl.ds(pl.multiple_of(at, ROWS), ROWS), :] = dot(
            hid_ref[...], w2_ref[...].reshape(parts * out_depth, dim)).astype(BF16)


def expert_backward_kernel(capacity, n_local, loc, meta, win_ref, x_ref, c_ref, gcol_ref, slots_ref,
                           w1_ref, w3_ref, w2_ref, dx_ref, dgate_ref, hid_ref, dg_ref, du_ref, all_ref, dcol_ref):
    step = pl.program_id(0)

    @pl.when(step == 0)
    def _():
        zero_all((all_ref, dcol_ref))

    @pl.when(step < meta[0])
    def _():
        block = pl.ds(pl.multiple_of(step * ROWS, ROWS), ROWS)
        rows = x_ref[...]
        grad = c_ref[...]
        gate = jnp.sum(gcol_ref[...], axis=1, keepdims=True)
        partial = jnp.zeros((ROWS, 128), F32)
        for at in range(0, w1_ref.shape[1], CHUNK):
            cols = slice(at, at + CHUNK)
            pre_gate = dot(rows, w1_ref[:, cols])
            pre_up = dot(rows, w3_ref[:, cols])
            sigma = jax.nn.sigmoid(pre_gate)
            hidden = (pre_gate * sigma * pre_up).astype(BF16)
            hid_ref[:, cols] = hidden
            back = dot(grad, w2_ref[cols, :], LAST)
            product = hidden.astype(F32) * back
            for lane in range(0, CHUNK, 128):
                partial += product[:, lane:lane + 128]
            dg_ref[:, cols], du_ref[:, cols] = swiglu_grads(pre_gate, pre_up, sigma, back * gate)
        dcol_ref[block, :] = partial
        all_ref[block, :] = (dot(dg_ref[...], w1_ref[...], LAST) + dot(du_ref[...], w3_ref[...], LAST)).astype(BF16)

    @pl.when(step == pl.num_programs(0) - 1)
    def _():
        spread(meta, all_ref, dx_ref, capacity)
        line = lax.broadcasted_iota(jnp.int32, (WIN, SUB), 0)
        n_src, n_tok = dgate_ref.shape
        for src in range(n_src):
            def body(sub, _):
                window = (src * (n_tok // SUB) + sub) * n_local + loc
                part = pl.ds(pl.multiple_of(sub * SUB, SUB), SUB)
                where = slots_ref[src:src + 1, part] - win_ref[2 * window]
                source = pl.ds(pl.multiple_of(win_ref[2 * window + 1], 16), WIN)
                values = jnp.sum(dcol_ref[source, :], axis=1, keepdims=True)
                dgate_ref[src:src + 1, part] = jnp.sum(jnp.where(line == where, values, 0.0), axis=0, keepdims=True)
                return 0

            lax.fori_loop(0, n_tok // SUB, body, 0)


def expert_weights_kernel(n_alias, meta, x_ref, c_ref, gcol_ref, hid_ref, dg_ref, du_ref, *refs):
    dw1_ref, dw3_ref, dw2_ref = refs[n_alias:]
    step = pl.program_id(0)

    @pl.when(step == 0)
    def _():
        zero_all((dw1_ref, dw3_ref, dw2_ref))

    @pl.when(step < meta[0])
    def _():
        gate = jnp.sum(gcol_ref[...], axis=1, keepdims=True)
        scaled = (c_ref[...].astype(F32) * gate).astype(BF16)
        rows = x_ref[...]
        dw1_ref[...] += dot(rows, dg_ref[...], FIRST)
        dw3_ref[...] += dot(rows, du_ref[...], FIRST)
        dw2_ref[...] += dot(hid_ref[...], scaled, FIRST)


def solution(mesh):
    group = mesh.shape['ep']
    tok_spec = P(('dp', 'ep'), None)
    exp_spec = P('ep', None, None)
    full_spec = P(None, None)
    grad_spec = P(('dp', 'ep'), None, None)
    buffered = pl.Buffered(buffer_count=1)

    def layer_program(x_in, grad_y, ids_a, gate_a, ids_b, gate_b, w1_a, w3_a, w2_a, w1_b, w3_b, w2_b,
                       wg_mid, wu_mid, wd_mid, wg_top, wu_top, wd_top):
        n_tok, dim = x_in.shape
        n_local, _, ff = w1_a.shape
        n_exp = n_local * group
        capacity = 2 * n_tok * ids_a.shape[1] // n_exp
        n_rows = group * capacity
        me = lax.axis_index('ep')

        tile = pl.BlockSpec((TOK, dim), lambda i, *_: (i, 0))
        col_tile = pl.BlockSpec((TOK, n_exp), lambda i, *_: (i, 0))
        whole = pl.BlockSpec((n_rows, dim), lambda i, *_: (0, 0), pipeline_mode=buffered)
        pair_rows = pl.BlockSpec((n_exp * capacity, dim), lambda i, *_: (0, 0), pipeline_mode=buffered)
        w_in = pl.BlockSpec((dim, ff), lambda i, *_: (0, 0), pipeline_mode=buffered)
        w_out = pl.BlockSpec((ff, dim), lambda i, *_: (0, 0), pipeline_mode=buffered)
        rows_shape = jax.ShapeDtypeStruct((n_tok, dim), BF16)
        buffer_shape = jax.ShapeDtypeStruct((n_rows, dim), BF16)
        wide = pltpu.VMEM((TOK, ff), BF16)
        narrow = pltpu.VMEM((TOK, dim), BF16)
        unit_flops = 2 * n_tok * dim * ff

        def token_call(kernel, in_specs, out_specs, out_shape, scratch, matmuls):
            return pl.pallas_call(
                functools.partial(kernel, capacity),
                grid_spec=pltpu.PrefetchScalarGridSpec(
                    num_scalar_prefetch=1, grid=(n_tok // TOK,), in_specs=in_specs, out_specs=out_specs,
                    scratch_shapes=scratch),
                out_shape=out_shape, compiler_params=params(),
                cost_estimate=cost(int(matmuls * unit_flops), 20 * 2**20))

        forward = token_call(forward_kernel, [tile, col_tile, col_tile, whole, whole, w_in, w_in, w_out],
                             [tile, tile], [rows_shape, rows_shape], [wide], 5)
        top = token_call(top_kernel, [tile, tile, col_tile, col_tile, pair_rows, w_in, w_in, w_out],
                         [tile, tile], [rows_shape, rows_shape], [wide, wide, wide, narrow], 8)
        backward = token_call(backward_kernel, [tile, tile, col_tile, whole, whole, w_in, w_in, w_out],
                              tile, rows_shape, [wide, wide, narrow], 7)
        final = token_call(final_kernel, [tile, col_tile, whole, whole], tile, rows_shape, [], 1)

        n_blocks = n_rows // ROWS
        tiles = n_tok // PACK
        pack_tile = pl.BlockSpec((PACK, dim), lambda i, *_: (i, 0))
        line = pl.BlockSpec((None, n_local, PACK), lambda i, *_: (i // tiles, 0, i % tiles))
        column_shape = jax.ShapeDtypeStruct((n_rows, 128), F32)
        column = pl.BlockSpec((n_rows, 128), lambda i, *_: (0, 0), pipeline_mode=buffered)

        def pack(windows, tokens, slots, gates=None):
            with_gates = gates is not None
            return pl.pallas_call(
                functools.partial(pack_kernel, n_local, n_local, with_gates),
                grid_spec=pltpu.PrefetchScalarGridSpec(
                    num_scalar_prefetch=1, grid=(group * tiles,),
                    in_specs=[pack_tile, line] + [line] * with_gates,
                    out_specs=[whole] * n_local + [column] * (n_local * with_gates)),
                out_shape=[buffer_shape] * n_local + [column_shape] * (n_local * with_gates),
                compiler_params=params(), cost_estimate=cost(2 * unit_flops, 20 * 2**20),
            )(windows, tokens, slots, *((gates,) if with_gates else ()))

        def row_block(i, meta, *_):
            return (jnp.maximum(jnp.minimum(i, meta[0] - 1), 0), 0)

        def expert_specs(loc):
            return (pl.BlockSpec((ROWS, dim), row_block),
                    pl.BlockSpec((None, dim, ff), lambda i, *_: (loc, 0, 0), pipeline_mode=buffered),
                    pl.BlockSpec((None, ff, dim), lambda i, *_: (loc, 0, 0), pipeline_mode=buffered))

        def expert_forward(loc, meta, tokens, w1, w3, w2):
            block, e_in, e_out = expert_specs(loc)
            return pl.pallas_call(
                functools.partial(expert_forward_kernel, capacity),
                grid_spec=pltpu.PrefetchScalarGridSpec(
                    num_scalar_prefetch=1, grid=(n_blocks,), in_specs=[block, e_in, e_in, e_out], out_specs=whole,
                    scratch_shapes=[pltpu.VMEM((n_rows, dim), BF16), pltpu.VMEM((ROWS, ff), BF16)]),
                out_shape=buffer_shape, compiler_params=params(),
                cost_estimate=cost(3 * unit_flops, 12 * 2**20))(meta, tokens, w1, w3, w2)

        hidden_block = pl.BlockSpec((ROWS, ff), row_block)
        hidden_shape = jax.ShapeDtypeStruct((n_rows, ff), BF16)

        def expert_backward(loc, meta, windows, tokens, grads, gates, slots, w1, w3, w2):
            block, e_in, e_out = expert_specs(loc)
            small = pl.BlockSpec((group, n_tok), lambda i, *_: (0, 0), pipeline_mode=buffered)
            return pl.pallas_call(
                functools.partial(expert_backward_kernel, capacity, n_local, loc),
                grid_spec=pltpu.PrefetchScalarGridSpec(
                    num_scalar_prefetch=2, grid=(n_blocks,),
                    in_specs=[block, block, pl.BlockSpec((ROWS, 128), row_block), small, e_in, e_in, e_out],
                    out_specs=[whole, small] + [hidden_block] * 3,
                    scratch_shapes=[pltpu.VMEM((n_rows, dim), BF16), pltpu.VMEM((n_rows, 128), F32)]),
                out_shape=[buffer_shape, jax.ShapeDtypeStruct((group, n_tok), F32)] + [hidden_shape] * 3,
                compiler_params=params(), cost_estimate=cost(5 * unit_flops, 60 * 2**20),
            )(meta, windows, tokens, grads, gates, slots, w1, w3, w2)

        def expert_weights(loc, meta, tokens, grads, gates, hidden, earlier):
            block, e_in, e_out = expert_specs(loc)
            n_alias = 0 if earlier is None else 3
            aliases = {} if earlier is None else {7: 0, 8: 1, 9: 2}
            extra = () if earlier is None else tuple(earlier)
            return pl.pallas_call(
                functools.partial(expert_weights_kernel, n_alias),
                grid_spec=pltpu.PrefetchScalarGridSpec(
                    num_scalar_prefetch=1, grid=(n_blocks,),
                    in_specs=([block, block, pl.BlockSpec((ROWS, 128), row_block)] + [hidden_block] * 3
                              + [pl.BlockSpec(memory_space=pl.ANY)] * n_alias),
                    out_specs=[e_in, e_in, e_out]),
                out_shape=[jax.ShapeDtypeStruct((n_local, dim, ff), F32), jax.ShapeDtypeStruct((n_local, dim, ff), F32),
                           jax.ShapeDtypeStruct((n_local, ff, dim), F32)],
                input_output_aliases=aliases, compiler_params=params(),
                cost_estimate=cost(3 * unit_flops, 60 * 2**20),
            )(meta, tokens, grads, gates, *hidden, *extra)

        parts = mesh.shape['dp']
        pair_shape = jax.ShapeDtypeStruct((n_exp * capacity, dim), BF16)
        max_steps = n_tok * ids_a.shape[1] // ROWS + n_exp

        def pack_pairs(windows, tokens, slots):
            return pl.pallas_call(
                functools.partial(pack_kernel, n_exp, 1, False),
                grid_spec=pltpu.PrefetchScalarGridSpec(
                    num_scalar_prefetch=1, grid=(tiles,),
                    in_specs=[pack_tile, pl.BlockSpec((n_exp, PACK), lambda i, *_: (0, i))], out_specs=[pair_rows]),
                out_shape=[pair_shape], compiler_params=params(), cost_estimate=cost(2 * unit_flops, 12 * 2**20),
            )(windows, tokens, slots)[0]

        def all_experts(plan, pairs, w1, w3, w2):
            def pair_block(i, plan):
                return (plan[1 + 2 * i] * (capacity // ROWS) + plan[2 + 2 * i], 0)

            def weights(w):
                return pl.BlockSpec((parts, None, None) + w.shape[3:],
                                    lambda i, plan: (0, plan[1 + 2 * i] // n_local, plan[1 + 2 * i] % n_local, 0, 0))

            return pl.pallas_call(
                functools.partial(all_experts_kernel, capacity),
                grid_spec=pltpu.PrefetchScalarGridSpec(
                    num_scalar_prefetch=1, grid=(max_steps,),
                    in_specs=[pl.BlockSpec((ROWS, dim), pair_block), weights(w1), weights(w3), weights(w2)],
                    out_specs=pair_rows, scratch_shapes=[pltpu.VMEM((ROWS, ff), BF16)]),
                out_shape=pair_shape, compiler_params=params(),
                cost_estimate=cost(6 * unit_flops, 60 * 2**20))(plan, pairs, w1, w3, w2)

        def block_plan(counts):
            blocks = (counts + ROWS - 1) // ROWS
            ends = jnp.cumsum(blocks)
            index = jnp.minimum(jnp.arange(max_steps, dtype=jnp.int32), ends[-1] - 1)
            passed = (index[:, None] >= ends[None, :]).astype(jnp.int32)
            expert = jnp.sum(passed, axis=1)
            block = index - jnp.sum(passed * blocks[None, :], axis=1)
            return jnp.concatenate([ends[-1:], jnp.stack([expert, block], axis=1).reshape(-1)])

        def gather_weights(w):
            depth = w.shape[1] // parts
            mine = lax.dynamic_slice_in_dim(w, lax.axis_index('dp') * depth, depth, 1)
            return lax.all_gather(mine, ('dp', 'ep')).reshape((parts, group) + mine.shape)

        ids_both, gates_both = jnp.stack([ids_a, ids_b]), jnp.stack([gate_a, gate_b])
        slots_here, gates_here, starts_here, counts_here = route(ids_both, gates_both, jnp.arange(n_exp, dtype=jnp.int32))
        windows_here = jnp.minimum(starts_here // 16 * 16, capacity - WIN)
        win_a, win_b = windows_here.transpose(0, 2, 1).reshape(2, -1)
        base_b = (jnp.arange(n_exp, dtype=jnp.int32) * capacity)[:, None]
        win_pairs = jnp.stack([windows_here[1], windows_here[1] + base_b], axis=-1).transpose(1, 0, 2).reshape(-1)
        plan_b = block_plan(counts_here[1])
        slots_col, gates_col = slots_here.transpose(0, 2, 1), gates_here.transpose(0, 2, 1)
        ids_all = lax.all_gather(ids_both, 'ep')
        gates_all = lax.all_gather(gates_both, 'ep')
        slots, gates, starts, counts = route(ids_all, gates_all, me * n_local + jnp.arange(n_local, dtype=jnp.int32))
        room = (counts + 15) // 16 * 16
        offsets = jnp.cumsum(room, axis=0) - room
        windows = jnp.minimum(starts // 16 * 16, capacity - WIN)
        windows = jnp.stack([windows, windows + offsets[..., None]], axis=-1)
        windows = windows.transpose(1, 0, 3, 2, 4).reshape(2, -1)
        n_used = (jnp.sum(room, axis=0) + ROWS - 1) // ROWS
        meta = jnp.concatenate([n_used[None], offsets], axis=0)

        def gather_rows(rows):
            return lax.all_gather(rows, 'ep', axis=0, tiled=True)

        def to_home(rows):
            return lax.all_to_all(rows.reshape(group, capacity, dim), 'ep', 0, 0, tiled=True).reshape(n_rows, dim)

        def moe_forward(tokens, layer, w1, w3, w2):
            backs = []
            for loc in range(n_local):
                rows = expert_forward(loc, meta[:, layer, loc], tokens[loc], w1, w3, w2)
                if backs:
                    rows, backs[-1] = lax.optimization_barrier((rows, backs[-1]))
                backs.append(to_home(rows))
            return backs

        def moe_backward(tokens, grads, layer, ids, w1, w3, w2):
            backs, dgates, kept, earlier = [], [], [], None
            packed = pack(windows[layer], grads, slots[:, layer], gates[:, layer])
            for loc in range(n_local):
                dx, dgate, *hidden = expert_backward(
                    loc, meta[:, layer, loc], windows[layer], tokens[loc], packed[loc], packed[n_local + loc],
                    slots[:, layer, loc], w1, w3, w2)
                if backs:
                    dx, backs[-1] = lax.optimization_barrier((dx, backs[-1]))
                backs.append(to_home(dx))
                dgates.append(dgate)
                kept.append(hidden)
            for loc in range(n_local):
                earlier = expert_weights(loc, meta[:, layer, loc], tokens[loc], packed[loc], packed[n_local + loc],
                                         kept[loc], earlier)
            dgates, backs = lax.optimization_barrier((jnp.stack(dgates, axis=1), backs))
            home = lax.all_to_all(dgates, 'ep', 0, 0, tiled=True)
            experts = jnp.arange(n_exp, dtype=jnp.int32)[:, None, None]
            dgate = jnp.sum(jnp.where(ids[None] == experts, home.reshape(n_exp, n_tok)[:, :, None], 0.0), axis=0)
            return backs, dgate, earlier

        x_all = gather_rows(x_in)
        x_all, windows, *own_b = lax.optimization_barrier((x_all, windows, w1_b, w3_b, w2_b))
        all_b = [gather_weights(w) for w in own_b]
        tokens_a = pack(windows[0], x_all, slots[:, 0])
        backs_a = moe_forward(tokens_a, 0, w1_a, w3_a, w2_a)
        x_a, x_mid = forward(win_a, x_in, slots_col[0], gates_col[0], *backs_a, wg_mid, wu_mid, wd_mid)
        pairs_b = all_experts(plan_b, pack_pairs(win_pairs, x_mid, slots_here[1]), *all_b)

        y_out, grad_b = top(win_b, x_mid, grad_y, slots_col[1], gates_col[1], pairs_b, wg_top, wu_top, wd_top)
        tokens_b = pack(windows[1], gather_rows(x_mid), slots[:, 1])
        again, _ = lax.optimization_barrier((x_in, grad_b))
        backs_b, dgate_b, dw_b = moe_backward(tokens_b, gather_rows(grad_b), 1, ids_b, w1_b, w3_b, w2_b)
        tokens_a = pack(windows[0], gather_rows(again), slots[:, 0])
        grad_a = backward(win_b, grad_b, x_a, slots_col[1], *backs_b, wg_mid, wu_mid, wd_mid)
        backs_a, dgate_a, dw_a = moe_backward(tokens_a, gather_rows(grad_a), 0, ids_a, w1_a, w3_a, w2_a)
        dx_in = final(win_a, grad_a, slots_col[0], *backs_a)
        return (y_out, dx_in, *dw_a, *dw_b, dgate_a, dgate_b)

    in_specs = (tok_spec, tok_spec, tok_spec, tok_spec, tok_spec, tok_spec,
                exp_spec, exp_spec, exp_spec, exp_spec, exp_spec, exp_spec,
                full_spec, full_spec, full_spec, full_spec, full_spec, full_spec)
    out_specs = (tok_spec, tok_spec, grad_spec, grad_spec, grad_spec, grad_spec, grad_spec, grad_spec, tok_spec, tok_spec)
    return jax.shard_map(layer_program, mesh=mesh, in_specs=in_specs, out_specs=out_specs, check_vma=False)
```
